32 devices in a mesh: groups: 2 (over x), kv: 16 (over z, y, core).
Axes of the slice: x: 2, y: 2, z: 4, core: 2. Of those that a mesh axis runs over, the one named last changes fastest.
Arguments:
- queries: bfloat16 [80, 18432], P('groups', 'kv'), parts along dimension 0, may hold values from -240 to 240
- latent_cache: bfloat16 [80, 2048, 576], P('groups', 'kv'), parts along dimension 0, may hold values from -6 to 6
- context_lengths: int32 [80], P('groups'), parts along dimension 0, may hold values from 128 to 2048, as said below
- value_up: bfloat16 [16384, 128], P('kv'), may hold values from -0.25 to 0.25
- out_proj: bfloat16 [4096, 7168], P('kv'), may hold values from -0.09375 to 0.09375
- residual: bfloat16 [80, 7168], P('groups', 'kv'), parts along dimension 0, may hold values from -0.75 to 0.75
- norm_gain: bfloat16 [7168], P('kv'), may hold values from 0.5 to 1.5
- expert_ids: int32 [80, 8], P('groups'), parts along dimension 0, may hold values from 0 to 255, all different within a row; in each aligned block of 40 rows (0 to 39, 40 to 79, ...) at most 2 rows name the same one
- gate_weights: float32 [80, 8], P('groups'), parts along dimension 0, may hold values from 0.05 to 0.5
Outputs:
- dispatched: bfloat16 [512, 2, 7168], P(('groups', 'kv')), parts along dimension 0
- slot_scale: float32 [512, 2], P(('groups', 'kv')), parts along dimension 0
- slot_gate: float32 [512, 2], P(('groups', 'kv')), parts along dimension 0
The draws below stay inside these ranges and needn't reach their ends.
There are 2 independent parts, one for each index of `groups`. The reference program is written for one: setup_inputs(seed, part) draws one part's arguments, and reference() takes and returns one part's arrays. A program takes and returns all parts, laid end to end along the dimension named above; an argument that names none is the same for every part. Nothing has to cross between parts.
Inputs may be any that keep to these rules, and one draw needn't show every extreme that they name: `context_lengths`: multiples of 128; some sequence is 2048 long. `expert_ids`: each token names 8 different experts; no expert is named by more than 2 tokens, a bound that some block reaches.
All inputs are finite; a program needn't handle non-finite values. Where the reference program divides by a largest or mean magnitude, that divisor is 1e-20 or more.
Results may differ from the reference program's by a relative error of at most 0.0069.
Values may be sent and summed in bfloat16 or wider, within the bound.
No kernel may reach another device: no remote copies, remote signals or barrier semaphores. Data moves between devices by JAX's collectives and lax.ppermute only.
A program may use at most 64 MiB of HBM per device.

```python
import math
import jax
import jax.numpy as jnp
import numpy as np
from jax import lax

H = 32
LAT = 512
ROPE = 64
VD = 128
D = 7168
EXPERTS = 256
TOPK = 8
SEQS = 40
CTX_DEV = 128
BLOCK = 128
CTX = 2048
CAP = 2
N_KV = 16


def draw_queries(key, part):
    base_key = jax.random.fold_in(jax.random.fold_in(key, 11), 0)
    values = jnp.clip(jax.random.normal(base_key, (SEQS, H, LAT + ROPE), jnp.float32), -6.0, 6.0)
    return values.reshape(SEQS, H * (LAT + ROPE)).astype(jnp.bfloat16)


def draw_context_lengths(key, part):
    count_key, pick_key = jax.random.split(jax.random.fold_in(key, 7))
    blocks = jax.random.randint(count_key, (SEQS,), 1, CTX // BLOCK + 1)
    longest = jax.random.randint(pick_key, (), 0, SEQS)
    blocks = jnp.where(jnp.arange(SEQS) == longest, CTX // BLOCK, blocks)
    return (blocks * BLOCK).astype(jnp.int32)


def level_of(key, shape, cuts, least, high):
    def one(axis_at, shards_of):
        steps = jax.random.uniform(jax.random.fold_in(jax.random.fold_in(key, 6), axis_at), (shards_of,), jnp.float32, least / len(cuts), high / len(cuts))
        return jnp.repeat(jnp.exp(steps), shape[axis_at] // shards_of).reshape((-1,) + (1,) * (len(shape) - axis_at - 1))

    level = one(*cuts[0])
    for cut in cuts[1:]:
        level = level * one(*cut)
    return level


def assign_block(rng, own, number, rows, number_of, top, limit, skew):
    ranking = jax.random.permutation(rng, number_of)
    heavy_load, ordinary = shares(number_of, rows * top, limit, skew, True), shares(number_of, rows * top, limit, skew, False)
    places = jnp.arange(number_of)

    def named(lengths, rotation):
        used = int((lengths > 0).sum())
        fixed = max(1, used // 4)
        moved = fixed + (places - fixed + rotation * (used - fixed)) % max(1, number_of - fixed)
        return jnp.zeros((number_of,), jnp.int32).at[ranking[jnp.where(places < fixed, places, moved)]].set(jnp.asarray(lengths, jnp.int32))

    lengths = jnp.where(number % 4 == 0, named(heavy_load, number // 4), named(ordinary, number - number // 4 - 1))
    mixed = jax.random.permutation(jax.random.fold_in(own, 3), number_of)
    giver, sink = mixed[0:number_of // 2 * 2:2], mixed[1:number_of // 2 * 2:2]
    margin = jnp.minimum(lengths[giver] - 1, limit - lengths[sink]) // 2
    margin = jnp.where((giver == ranking[0]) | (sink == ranking[0]) | (lengths[sink] == 0), 0, jnp.maximum(margin, 0))
    moved = jax.random.randint(jax.random.fold_in(own, 4), (number_of // 2,), 0, 1 << 20) % (margin + 1)
    lengths = lengths.at[giver].add(-moved).at[sink].add(moved)
    labels = jnp.searchsorted(jnp.cumsum(lengths), jnp.arange(rows * top), side="right").astype(jnp.int32)
    listing = labels.reshape(top, rows).T
    listing = listing[jax.random.permutation(jax.random.fold_in(own, 1), rows)]
    rotation = jax.random.randint(jax.random.fold_in(own, 2), (rows, 1), 0, top)
    return jnp.take_along_axis(listing, (jnp.arange(top)[None, :] + rotation) % top, axis=1)


def shares(count, total, most, skew, full):
    loads = [(1 << 20) // math.isqrt(grade ** skew) + 1 for grade in range(1, count + 1)]
    largest = most if full else min(most, max(-(-total // count), total * loads[0] // sum(loads)))
    least = 1 if total - largest >= count - 1 else 0
    holding, rest = [largest] + [least] * (count - 1), total - largest - least * (count - 1)
    while rest > 0:
        candidates = [i for i in range(1, count) if holding[i] < largest] or [i for i in range(1, count) if holding[i] < most]
        whole, left = sum([loads[i] for i in candidates]), rest
        for i in candidates:
            addition = min(most - holding[i], max(1, left * loads[i] // whole), rest)
            holding[i] = holding[i] + addition
            rest = rest - addition
    return np.array(holding)


def gaussian(stream_key, extent, scale, reach, cuts=(), held_as=jnp.bfloat16):
    loudness = level_of(stream_key, extent, cuts, -0.22, 0.18) if cuts else 1.0
    entries = jax.random.normal(stream_key, extent, jnp.float32) * scale * loudness
    return jnp.minimum(jnp.maximum(entries, -reach), reach).astype(held_as)


def setup_inputs(seed: int = 0, part: int = 0) -> dict:
    key_list = jax.random.split(jax.random.key(seed), 10)
    part_splits = jax.random.split(jax.random.fold_in(key_list[9], part), 10)
    queries = draw_queries(jax.random.fold_in(jax.random.fold_in(key_list[9], part), 71), part)
    latent_cache = gaussian(part_splits[1], (SEQS, CTX, LAT + ROPE), 1.0, 6.0, ((1, 16),))
    context_lengths = draw_context_lengths(jax.random.fold_in(jax.random.fold_in(key_list[9], part), 71), part)
    value_up = gaussian(key_list[3], (H * LAT, VD), LAT ** -0.5, 0.25, ((0, 16),))
    out_proj = gaussian(key_list[4], (H * VD, D), (H * VD) ** -0.5, 0.09375, ((0, 16),))
    residual = gaussian(part_splits[5], (SEQS, D), 0.05, 0.75, ((1, 16),))
    norm_gain = jnp.clip(1.0 + 0.1 * jax.random.normal(key_list[6], (D,), jnp.float32), 0.5, 1.5).astype(jnp.bfloat16)
    expert_ids_keys = jax.random.split(jax.random.fold_in(part_splits[7], 1), SEQS // SEQS)
    expert_ids_turns = jax.random.permutation(jax.random.fold_in(part_splits[7], 3), SEQS // SEQS)
    expert_ids = jax.vmap(lambda own, number: assign_block(jax.random.fold_in(part_splits[7], 2), own, number, SEQS, EXPERTS, TOPK, CAP, 2))(expert_ids_keys, expert_ids_turns).reshape((SEQS, TOPK))
    gate_weights = jnp.clip(jax.random.uniform(part_splits[8], (SEQS, TOPK), jnp.float32, 0.05, 0.5), 0.05, 0.5)
    return dict(queries=queries, latent_cache=latent_cache, context_lengths=context_lengths, value_up=value_up, out_proj=out_proj, residual=residual, norm_gain=norm_gain, expert_ids=expert_ids, gate_weights=gate_weights)


score_scale = 192.0 ** (-0.5)
masked_score = -1e+30
small_eps = 1e-06

def slot_targets(expert_ids):
    flat_ids = expert_ids.reshape(-1).astype(jnp.int32)
    order_index = jnp.arange(flat_ids.shape[0], dtype=jnp.int32)
    same_before = (flat_ids[:, None] == flat_ids[None, :]) & (order_index[None, :] < order_index[:, None])
    rank_within = lax.optimization_barrier(jnp.sum(same_before.astype(jnp.int32), axis=1)).astype(jnp.int32)
    return flat_ids * CAP + rank_within

def reference(queries, latent_cache, context_lengths, value_up, out_proj, residual, norm_gain, expert_ids, gate_weights):
    query_rows = queries.reshape(SEQS, H, LAT + ROPE).astype(jnp.float32)
    shards = latent_cache.reshape(SEQS, N_KV, CTX_DEV, LAT + ROPE)

    def shard_step(running, shard_index):
        run_max, run_total, run_out = running
        cache_block = lax.dynamic_index_in_dim(shards, shard_index, 1, keepdims=False).astype(jnp.float32)
        scores = jnp.einsum('shq,scq->shc', query_rows, cache_block, precision=lax.Precision.HIGHEST) * score_scale
        position = shard_index * CTX_DEV + jnp.arange(CTX_DEV, dtype=jnp.int32)
        valid_mask = (position[None, :] < context_lengths[:, None])[:, None, :]
        scores = jnp.where(valid_mask, scores, masked_score)
        local_max = lax.optimization_barrier(jnp.max(scores, axis=2))
        weights = jnp.where(valid_mask, jnp.exp(scores - local_max[:, :, None]), 0.0)
        local_total = lax.optimization_barrier(jnp.sum(weights, axis=2))
        rounded = lax.optimization_barrier(weights.astype(jnp.bfloat16)).astype(jnp.float32)
        local_out = jnp.einsum('shc,scl->shl', rounded, cache_block[:, :, :LAT], precision=lax.Precision.HIGHEST)
        new_max = jnp.maximum(run_max, local_max)
        old_scale = jnp.exp(run_max - new_max)
        new_scale = jnp.exp(local_max - new_max)
        run_total = run_total * old_scale + local_total * new_scale
        run_out = run_out * old_scale[:, :, None] + local_out * new_scale[:, :, None]
        return ((new_max, run_total, run_out), None)
    start_state = (jnp.full((SEQS, H), masked_score, jnp.float32), jnp.zeros((SEQS, H), jnp.float32), jnp.zeros((SEQS, H, LAT), jnp.float32))
    final_state, unused = lax.scan(shard_step, start_state, jnp.arange(N_KV, dtype=jnp.int32))
    run_max, run_total, run_out = final_state
    merged = run_out / run_total[:, :, None]
    projector = value_up.reshape(H, LAT, VD).astype(jnp.float32)
    value_part = jnp.einsum('shl,hlv->shv', merged, projector, precision=lax.Precision.HIGHEST)
    value_rows = value_part.astype(jnp.bfloat16).reshape(SEQS, H * VD)
    attn_rows = jnp.dot(value_rows, out_proj, preferred_element_type=jnp.float32)
    summed = attn_rows + residual.astype(jnp.float32)
    inverse_rms = lax.rsqrt(lax.optimization_barrier(jnp.mean(summed * summed, axis=1)) + small_eps)
    normed = summed * inverse_rms[:, None] * norm_gain.astype(jnp.float32)
    peak_abs = lax.optimization_barrier(jnp.max(jnp.abs(normed), axis=1)) + small_eps
    coded_rows = (normed / peak_abs[:, None]).astype(jnp.bfloat16)
    targets = slot_targets(expert_ids)
    owner = jnp.arange(SEQS * TOPK, dtype=jnp.int32) // TOPK
    dispatched = jnp.zeros((EXPERTS * CAP, D), jnp.bfloat16).at[targets].set(coded_rows[owner])
    slot_scale = jnp.zeros((EXPERTS * CAP,), jnp.float32).at[targets].set(peak_abs[owner])
    slot_gate = jnp.zeros((EXPERTS * CAP,), jnp.float32).at[targets].set(gate_weights.reshape(-1))
    return (dispatched.reshape(EXPERTS, CAP, D), slot_scale.reshape(EXPERTS, CAP), slot_gate.reshape(EXPERTS, CAP))
```

```python
import jax
import jax.numpy as jnp
from jax import lax
from jax.experimental import pallas as pl
from jax.experimental.pallas import tpu as pltpu
from jax.sharding import PartitionSpec as P

H = 32
LAT = 512
ROPE = 64
VD = 128
D = 7168
EXPERTS = 256
TOPK = 8
CAP = 2


score_scale = 192.0 ** (-0.5)
masked_score = -1e30
small_eps = 1e-06


def from_partner(value, axis, bit):
    mask = 2**bit
    pairs = [(source, source ^ mask) for source in range(lax.axis_size(axis))]
    return lax.ppermute(value, axis, pairs)


def slot_targets(expert_ids):
    flat_ids = expert_ids.reshape(-1)
    order_index = jnp.arange(flat_ids.shape[0], dtype=jnp.int32)
    same_before = (flat_ids[:, None] == flat_ids[None, :]) & (
        order_index[None, :] < order_index[:, None]
    )
    rank_within = jnp.sum(same_before.astype(jnp.int32), axis=1)
    return flat_ids * CAP + rank_within


def slot_match(targets, first_slot, slot_count):
    slot_index = first_slot + jnp.arange(slot_count, dtype=jnp.int32)
    return (slot_index[:, None] == targets[None, :]).astype(jnp.float32)


def token_picker(matches, seq_count):
    return jnp.sum(matches.reshape(matches.shape[0], seq_count, TOPK), axis=2)


def split_heads(
    queries,
    latent_cache,
    context_lengths,
    value_up,
    out_proj,
    residual,
    norm_gain,
    expert_ids,
    gate_weights,
):
    kv_count = lax.axis_size("kv")
    shard_index = lax.axis_index("kv")
    seq_count = queries.shape[0]
    query_rows = lax.all_gather(queries, "kv", axis=1, tiled=True).reshape(seq_count, H, LAT + ROPE)
    ctx_local = latent_cache.shape[1]
    scores = (
        jnp.einsum("shq,scq->shc", query_rows, latent_cache, preferred_element_type=jnp.float32)
        * score_scale
    )
    position = shard_index * ctx_local + jnp.arange(ctx_local, dtype=jnp.int32)
    valid_mask = (position[None, :] < context_lengths[:, None])[:, None, :]
    scores = jnp.where(valid_mask, scores, masked_score)
    local_max = jnp.max(scores, axis=2)
    weights = jnp.where(valid_mask, jnp.exp(scores - local_max[:, :, None]), 0.0)
    local_total = jnp.sum(weights, axis=2)
    local_out = jnp.einsum(
        "shc,scl->shl",
        weights.astype(jnp.bfloat16),
        latent_cache[:, :, :LAT],
        preferred_element_type=jnp.float32,
    )
    out_rows = out_proj.shape[0]
    col_count = H * LAT // kv_count
    segment = min(col_count, LAT)
    head_count = col_count // segment
    head_start = shard_index * col_count // LAT
    global_max = lax.pmax(local_max, "kv")
    scaling = jnp.exp(local_max - global_max)
    weight_total = lax.psum(local_total * scaling, "kv")
    scaled = (local_out * scaling[:, :, None]).reshape(seq_count, H * LAT)
    merged_sum = lax.psum_scatter(scaled, "kv", scatter_dimension=1, tiled=True).reshape(
        seq_count, head_count, segment
    )
    own_total = lax.dynamic_slice_in_dim(weight_total, head_start, head_count, 1)
    merged = merged_sum / own_total[:, :, None]
    projector = value_up.reshape(head_count, segment, VD).astype(jnp.float32)
    value_part = jnp.einsum("shl,hlv->shv", merged, projector, precision=lax.Precision.HIGHEST)
    holders = kv_count // H if kv_count > H else 1
    for bit in range(holders.bit_length() - 1):
        value_part = value_part + from_partner(value_part, "kv", bit)
    value_rows = value_part.astype(jnp.bfloat16).reshape(seq_count, head_count * VD)
    if holders > 1:
        value_rows = lax.dynamic_slice_in_dim(
            value_rows, shard_index % holders * out_rows, out_rows, 1
        )
    partial_out = jnp.dot(value_rows, out_proj, preferred_element_type=jnp.float32)
    experts_local = EXPERTS // kv_count
    slot_count = experts_local * CAP
    targets = slot_targets(expert_ids)
    own_match = slot_match(targets, shard_index * slot_count, slot_count)
    own_pick = token_picker(own_match, seq_count)
    slot_gate = jnp.dot(own_match, gate_weights.reshape(-1), precision=lax.Precision.HIGHEST)
    attn_rows = lax.psum(partial_out, "kv")
    resid_rows, gain_cols = (
        lax.all_gather(residual, "kv", axis=1, tiled=True),
        lax.all_gather(norm_gain, "kv", axis=0, tiled=True),
    )
    summed = attn_rows + resid_rows.astype(jnp.float32)
    inverse_rms = lax.rsqrt(jnp.mean(summed * summed, axis=1) + small_eps)
    normed = summed * inverse_rms[:, None] * gain_cols.astype(jnp.float32)
    peak_abs = jnp.max(jnp.abs(normed), axis=1) + small_eps
    coded_rows = (normed / peak_abs[:, None]).astype(jnp.bfloat16)
    dispatched = jnp.dot(
        own_pick.astype(jnp.bfloat16), coded_rows, preferred_element_type=jnp.float32
    ).astype(jnp.bfloat16)
    slot_scale = jnp.dot(own_pick, peak_abs, precision=lax.Precision.HIGHEST)
    return (
        dispatched.reshape(experts_local, CAP, D),
        slot_scale.reshape(experts_local, CAP),
        slot_gate.reshape(experts_local, CAP),
    )


LANES = 128


def params():
    return pltpu.CompilerParams(vmem_limit_bytes=56 * 1024 * 1024)


def whole(count):
    return [pl.BlockSpec(memory_space=pltpu.VMEM) for _ in range(count)]


def reverse_bits(value, width):
    result = 0
    for _ in range(width):
        result = result * 2 + value % 2
        value //= 2
    return result


def split_three(values):
    high = values.astype(jnp.bfloat16).astype(jnp.float32)
    middle = (values - high).astype(jnp.bfloat16).astype(jnp.float32)
    return high, middle, values - high - middle


def spread_stats(values):
    high, middle, low = split_three(values)
    lane = lax.broadcasted_iota(jnp.int32, values.shape, values.ndim - 1)
    axis = values.ndim - 1
    parts = jnp.where(lane < 64, pltpu.roll(middle, 32, axis), pltpu.roll(low, 64, axis))
    return jnp.where(lane < 32, high, parts).astype(jnp.bfloat16)


def gather_stats(tile):
    tile = tile.astype(jnp.float32)
    axis = tile.ndim - 1
    return tile + pltpu.roll(tile, LANES - 32, axis) + pltpu.roll(tile, LANES - 64, axis)


def attend(place_ref, lengths_ref, own_ref, other_ref, cache_ref, keep_ref, send_ref, q_ref, o_ref):
    half, seqs, width = own_ref.shape
    blocks = 2 * half
    heads = H // blocks
    ctx_local = cache_ref.shape[1]
    for block in range(blocks):
        rows = own_ref[block] if block < half else other_ref[block - half]
        rows = rows.astype(jnp.float32)
        for tile in range(width // LANES):
            q_ref[tile, block * seqs : (block + 1) * seqs, :] = rows[
                :, tile * LANES : (tile + 1) * LANES
            ]
    first = place_ref[0] * ctx_local
    position = first + lax.broadcasted_iota(jnp.int32, (H, ctx_local), 1)
    lane = lax.broadcasted_iota(jnp.int32, (blocks, LANES), 1)
    entry = LAT + ROPE

    def step(seq, carry):
        mine = pl.ds(seq, blocks, stride=seqs)
        rows = jnp.concatenate([q_ref[t, mine, :] for t in range(width // LANES)], axis=1)
        query = jnp.concatenate(
            [rows[:, h * entry : (h + 1) * entry] for h in range(heads)], axis=0
        ).astype(jnp.bfloat16)
        keys = cache_ref[seq]
        scores = (
            lax.dot_general(
                query, keys, (((1,), (1,)), ((), ())), preferred_element_type=jnp.float32
            )
            * score_scale
        )
        valid = position < lengths_ref[seq]
        scores = jnp.where(valid, scores, masked_score)
        top = jnp.max(scores, axis=1, keepdims=True)
        weights = jnp.where(valid, jnp.exp(scores - top), 0.0)
        total = jnp.sum(weights, axis=1, keepdims=True)
        out = lax.dot_general(
            weights.astype(jnp.bfloat16),
            keys[:, :LAT],
            (((1,), (0,)), ((), ())),
            preferred_element_type=jnp.float32,
        )
        stats = jnp.zeros((blocks, LANES), jnp.float32)
        for h in range(heads):
            part = slice(h * blocks, (h + 1) * blocks)
            for t in range(LAT // LANES):
                o_ref[h * (LAT // LANES) + t, mine, :] = out[part, t * LANES : (t + 1) * LANES]
            stats = jnp.where(lane == 2 * h, top[part], stats)
            stats = jnp.where(lane == 2 * h + 1, total[part], stats)
        o_ref[heads * LAT // LANES, mine, :] = stats
        return carry

    lax.fori_loop(0, seqs, step, 0, unroll=4)
    chip = place_ref[0] // 2
    bits = half.bit_length() - 1
    for block in range(half):
        to = chip ^ reverse_bits(block, bits)
        at = block * seqs
        past = at + half * seqs
        last = heads * LAT // LANES
        for t in range(last):
            cols = slice(t * LANES, (t + 1) * LANES)
            keep_ref[to, :, cols] = o_ref[t, at : at + seqs, :]
            send_ref[to, :, cols] = o_ref[t, past : past + seqs, :].astype(jnp.bfloat16)
        keep_ref[to, :, heads * LAT :] = o_ref[last, at : at + seqs, :]
        send_ref[to, :, heads * LAT :] = spread_stats(o_ref[last, past : past + seqs, :])


def merge_pair(keep_ref, got_ref, out_ref):
    half, seqs, width = keep_ref.shape
    heads = (width - LANES) // LAT
    lane = lax.broadcasted_iota(jnp.int32, (seqs, LANES), 1)

    def step(block, carry):
        mine = keep_ref[block, :, heads * LAT :]
        theirs = gather_stats(got_ref[block, :, heads * LAT :])
        stats = jnp.zeros((seqs, LANES), jnp.float32)
        for h in range(heads):
            top_a, top_b = mine[:, 2 * h : 2 * h + 1], theirs[:, 2 * h : 2 * h + 1]
            sum_a, sum_b = mine[:, 2 * h + 1 : 2 * h + 2], theirs[:, 2 * h + 1 : 2 * h + 2]
            top = jnp.maximum(top_a, top_b)
            scale_a, scale_b = jnp.exp(top_a - top), jnp.exp(top_b - top)
            total = sum_a * scale_a + sum_b * scale_b
            cols = slice(h * LAT, (h + 1) * LAT)
            out_ref[block, :, cols] = (
                keep_ref[block, :, cols] * scale_a
                + got_ref[block, :, cols].astype(jnp.float32) * scale_b
            ).astype(jnp.bfloat16)
            stats = jnp.where(lane == 2 * h, top, stats)
            stats = jnp.where(lane == 2 * h + 1, total, stats)
        out_ref[block, :, heads * LAT :] = spread_stats(stats)
        return carry

    lax.fori_loop(0, half, step, 0, unroll=2)


def project(place_ref, got_ref, up_ref, proj_ref, keep_ref, send_ref):
    half, seqs, width = got_ref.shape
    heads = (width - LANES) // LAT
    stats = [gather_stats(got_ref[c, :, heads * LAT :]) for c in range(half)]
    values = []
    for h in range(heads):
        tops = [s[:, 2 * h : 2 * h + 1] for s in stats]
        top = tops[0]
        for t in tops[1:]:
            top = jnp.maximum(top, t)
        scales = [jnp.exp(t - top) for t in tops]
        total = sum(s[:, 2 * h + 1 : 2 * h + 2] * x for s, x in zip(stats, scales))
        merged = sum(
            got_ref[c, :, h * LAT : (h + 1) * LAT].astype(jnp.float32) * scales[c]
            for c in range(half)
        )
        merged = merged / total
        high = merged.astype(jnp.bfloat16)
        low = (merged - high.astype(jnp.float32)).astype(jnp.bfloat16)
        up = up_ref[h * LAT : (h + 1) * LAT, :]
        value = jnp.dot(high, up, preferred_element_type=jnp.float32)
        value = value + jnp.dot(low, up, preferred_element_type=jnp.float32)
        values.append(value.astype(jnp.bfloat16))
    rows = jnp.concatenate(values, axis=1)
    cols = proj_ref.shape[1] // half
    part = cols // 2
    pad = send_ref.shape[2] - part
    north = place_ref[0] % 2 == 1
    zeros = jnp.zeros((seqs, pad), jnp.float32)
    for c in range(half):
        out = jnp.dot(
            rows, proj_ref[:, c * cols : (c + 1) * cols], preferred_element_type=jnp.float32
        )
        even = jnp.concatenate([out[:, :part], zeros], axis=1)
        odd = jnp.concatenate([out[:, part:], zeros], axis=1)
        keep_ref[c] = jnp.where(north, odd, even)
        send_ref[c] = jnp.where(north, even, odd).astype(jnp.bfloat16)


def normalise(got_ref, residual_ref, gain_ref, out_ref):
    half, seqs, width = got_ref.shape
    part = residual_ref.shape[1]
    total = got_ref[0].astype(jnp.float32)
    for c in range(1, half):
        total = total + got_ref[c].astype(jnp.float32)
    summed = total[:, :part] + residual_ref[...].astype(jnp.float32)
    squares = jnp.sum(summed * summed, axis=1, keepdims=True)
    gained = summed * gain_ref[...].astype(jnp.float32)
    peak = jnp.max(jnp.abs(gained), axis=1, keepdims=True)
    pad = width - part
    lane = lax.broadcasted_iota(jnp.int32, (seqs, pad), 1)
    stats = jnp.zeros((seqs, pad), jnp.float32)
    for at, piece in enumerate(split_three(squares) + split_three(peak)):
        stats = jnp.where(lane == at, piece, stats)
    row = jnp.concatenate([gained, stats], axis=1).astype(jnp.bfloat16)
    for c in range(half):
        out_ref[c] = row


def finish(place_ref, own_ref, other_ref, pick_ref, out_ref, scale_ref):
    half, seqs, width = own_ref.shape
    cols = out_ref.shape[1] // half
    part = cols // 2
    north = place_ref[0] % 2 == 1
    squares = jnp.zeros((seqs, 1), jnp.float32)
    peak = jnp.zeros((seqs, 1), jnp.float32)
    for ref in (own_ref, other_ref):
        for c in range(half):
            stats = ref[c, :, part:].astype(jnp.float32)
            squares = squares + stats[:, 0:1] + stats[:, 1:2] + stats[:, 2:3]
            peak = jnp.maximum(peak, stats[:, 3:4] + stats[:, 4:5] + stats[:, 5:6])
    inverse_rms = lax.rsqrt(squares / (cols * half) + small_eps)
    peak = peak * inverse_rms + small_eps
    factor = inverse_rms / peak
    pick = pick_ref[...]
    scale_ref[...] = jnp.sum(
        jnp.where(pick > 0, 1.0, 0.0)
        * jnp.transpose(jnp.broadcast_to(peak, (seqs, LANES)), (1, 0))[:1, :],
        axis=1,
        keepdims=True,
    )
    for c in range(half):
        own, other = own_ref[c, :, :part], other_ref[c, :, :part]
        pair = jnp.concatenate(
            [jnp.where(north, other, own), jnp.where(north, own, other)], axis=1
        )
        coded = (pair.astype(jnp.float32) * factor).astype(jnp.bfloat16)
        out_ref[:, c * cols : (c + 1) * cols] = jnp.dot(
            pick, coded, preferred_element_type=jnp.float32
        ).astype(jnp.bfloat16)


def whole_heads(
    queries,
    latent_cache,
    context_lengths,
    value_up,
    out_proj,
    residual,
    norm_gain,
    expert_ids,
    gate_weights,
):
    kv_count = lax.axis_size("kv")
    shard_index = lax.axis_index("kv")
    half = kv_count // 2
    seq_count, width = queries.shape
    place = shard_index.reshape(1).astype(jnp.int32)
    chips = [[2 * c + core for c in range(half)] for core in range(2)]
    smem = pl.BlockSpec(memory_space=pltpu.SMEM)

    def across_chips(value):
        return lax.all_to_all(value, "kv", 0, 0, axis_index_groups=chips, tiled=True)

    gathered = queries.reshape(1, seq_count, width)
    for bit in reversed(range(1, kv_count.bit_length() - 1)):
        gathered = jnp.concatenate([gathered, from_partner(gathered, "kv", bit)], axis=0)
    other_core = from_partner(gathered, "kv", 0)

    payload = H * LAT // kv_count + LANES
    block = (half, seq_count, payload)
    keep, send = pl.pallas_call(
        attend,
        name="attend",
        out_shape=(
            jax.ShapeDtypeStruct(block, jnp.float32),
            jax.ShapeDtypeStruct(block, jnp.bfloat16),
        ),
        in_specs=[smem, smem] + whole(3),
        out_specs=tuple(whole(2)),
        scratch_shapes=[
            pltpu.VMEM((width // LANES, kv_count * seq_count, LANES), jnp.float32),
            pltpu.VMEM((payload // LANES, kv_count * seq_count, LANES), jnp.float32),
        ],
        compiler_params=params(),
    )(place, context_lengths, gathered, other_core, latent_cache)
    got = from_partner(send, "kv", 0)
    merged = pl.pallas_call(
        merge_pair,
        name="merge_pair",
        out_shape=jax.ShapeDtypeStruct(block, jnp.bfloat16),
        in_specs=whole(2),
        out_specs=whole(1)[0],
        compiler_params=params(),
    )(keep, got)
    got = across_chips(merged)

    part = out_proj.shape[1] // kv_count
    padded = (part + 6 + LANES - 1) // LANES * LANES
    strip = (half, seq_count, padded)
    keep, send = pl.pallas_call(
        project,
        name="project",
        out_shape=(
            jax.ShapeDtypeStruct(strip, jnp.float32),
            jax.ShapeDtypeStruct(strip, jnp.bfloat16),
        ),
        in_specs=[smem] + whole(3),
        out_specs=tuple(whole(2)),
        compiler_params=params(),
    )(place, got, value_up, out_proj)
    got = from_partner(send, "kv", 0)
    got = across_chips((keep + got.astype(jnp.float32)).astype(jnp.bfloat16))
    copies = pl.pallas_call(
        normalise,
        name="normalise",
        out_shape=jax.ShapeDtypeStruct(strip, jnp.bfloat16),
        in_specs=whole(3),
        out_specs=whole(1)[0],
        compiler_params=params(),
    )(got, residual, norm_gain.reshape(1, part))
    own = across_chips(copies)
    other = from_partner(own, "kv", 0)

    experts_local = EXPERTS // kv_count
    slot_count = experts_local * CAP
    targets = slot_targets(expert_ids)
    own_match = slot_match(targets, shard_index * slot_count, slot_count)
    own_pick = token_picker(own_match, seq_count)
    slot_gate = jnp.sum(own_match * gate_weights.reshape(1, -1), axis=1)
    dispatched, slot_scale = pl.pallas_call(
        finish,
        name="finish",
        out_shape=(
            jax.ShapeDtypeStruct((slot_count, out_proj.shape[1]), jnp.bfloat16),
            jax.ShapeDtypeStruct((slot_count, 1), jnp.float32),
        ),
        in_specs=[smem] + whole(3),
        out_specs=tuple(whole(2)),
        compiler_params=params(),
    )(place, own, other, own_pick.astype(jnp.bfloat16))
    return (
        dispatched.reshape(experts_local, CAP, out_proj.shape[1]),
        slot_scale.reshape(experts_local, CAP),
        slot_gate.reshape(experts_local, CAP),
    )


def per_device(*args):
    if lax.axis_size("kv") > H:
        return split_heads(*args)
    return whole_heads(*args)


def solution(mesh):
    in_specs = (
        P("groups", "kv"),
        P("groups", "kv", None),
        P("groups"),
        P("kv", None),
        P("kv", None),
        P("groups", "kv"),
        P("kv"),
        P("groups", None),
        P("groups", None),
    )
    out_specs = (
        P(("groups", "kv"), None, None),
        P(("groups", "kv"), None),
        P(("groups", "kv"), None),
    )
    return jax.shard_map(
        per_device, mesh=mesh, in_specs=in_specs, out_specs=out_specs, check_vma=False
    )
```

```python
import jax
import jax.numpy as jnp
from jax import lax
from jax.experimental import pallas as pl
from jax.experimental.pallas import tpu as pltpu
from jax.sharding import PartitionSpec as P

H = 32
LAT = 512
ROPE = 64
VD = 128
D = 7168
EXPERTS = 256
TOPK = 8
CAP = 2


score_scale = 192.0 ** (-0.5)
masked_score = -1e30
small_eps = 1e-06


def from_partner(value, axis, bit):
    mask = 2**bit
    pairs = [(source, source ^ mask) for source in range(lax.axis_size(axis))]
    return lax.ppermute(value, axis, pairs)


def slot_targets(expert_ids):
    flat_ids = expert_ids.reshape(-1)
    order_index = jnp.arange(flat_ids.shape[0], dtype=jnp.int32)
    same_before = (flat_ids[:, None] == flat_ids[None, :]) & (
        order_index[None, :] < order_index[:, None]
    )
    rank_within = jnp.sum(same_before.astype(jnp.int32), axis=1)
    return flat_ids * CAP + rank_within


def slot_match(targets, first_slot, slot_count):
    slot_index = first_slot + jnp.arange(slot_count, dtype=jnp.int32)
    return (slot_index[:, None] == targets[None, :]).astype(jnp.float32)


def token_picker(matches, seq_count):
    return jnp.sum(matches.reshape(matches.shape[0], seq_count, TOPK), axis=2)


def split_heads(
    queries,
    latent_cache,
    context_lengths,
    value_up,
    out_proj,
    residual,
    norm_gain,
    expert_ids,
    gate_weights,
):
    kv_count = lax.axis_size("kv")
    shard_index = lax.axis_index("kv")
    seq_count = queries.shape[0]
    query_rows = lax.all_gather(queries, "kv", axis=1, tiled=True).reshape(seq_count, H, LAT + ROPE)
    ctx_local = latent_cache.shape[1]
    scores = (
        jnp.einsum("shq,scq->shc", query_rows, latent_cache, preferred_element_type=jnp.float32)
        * score_scale
    )
    position = shard_index * ctx_local + jnp.arange(ctx_local, dtype=jnp.int32)
    valid_mask = (position[None, :] < context_lengths[:, None])[:, None, :]
    scores = jnp.where(valid_mask, scores, masked_score)
    local_max = jnp.max(scores, axis=2)
    weights = jnp.where(valid_mask, jnp.exp(scores - local_max[:, :, None]), 0.0)
    local_total = jnp.sum(weights, axis=2)
    local_out = jnp.einsum(
        "shc,scl->shl",
        weights.astype(jnp.bfloat16),
        latent_cache[:, :, :LAT],
        preferred_element_type=jnp.float32,
    )
    out_rows = out_proj.shape[0]
    col_count = H * LAT // kv_count
    segment = min(col_count, LAT)
    head_count = col_count // segment
    head_start = shard_index * col_count // LAT
    global_max = lax.pmax(local_max, "kv")
    scaling = jnp.exp(local_max - global_max)
    weight_total = lax.psum(local_total * scaling, "kv")
    scaled = (local_out * scaling[:, :, None]).reshape(seq_count, H * LAT)
    merged_sum = lax.psum_scatter(scaled, "kv", scatter_dimension=1, tiled=True).reshape(
        seq_count, head_count, segment
    )
    own_total = lax.dynamic_slice_in_dim(weight_total, head_start, head_count, 1)
    merged = merged_sum / own_total[:, :, None]
    projector = value_up.reshape(head_count, segment, VD).astype(jnp.float32)
    value_part = jnp.einsum("shl,hlv->shv", merged, projector, precision=lax.Precision.HIGHEST)
    holders = kv_count // H if kv_count > H else 1
    for bit in range(holders.bit_length() - 1):
        value_part = value_part + from_partner(value_part, "kv", bit)
    value_rows = value_part.astype(jnp.bfloat16).reshape(seq_count, head_count * VD)
    if holders > 1:
        value_rows = lax.dynamic_slice_in_dim(
            value_rows, shard_index % holders * out_rows, out_rows, 1
        )
    partial_out = jnp.dot(value_rows, out_proj, preferred_element_type=jnp.float32)
    experts_local = EXPERTS // kv_count
    slot_count = experts_local * CAP
    targets = slot_targets(expert_ids)
    own_match = slot_match(targets, shard_index * slot_count, slot_count)
    own_pick = token_picker(own_match, seq_count)
    slot_gate = jnp.dot(own_match, gate_weights.reshape(-1), precision=lax.Precision.HIGHEST)
    attn_rows = lax.psum(partial_out, "kv")
    resid_rows, gain_cols = (
        lax.all_gather(residual, "kv", axis=1, tiled=True),
        lax.all_gather(norm_gain, "kv", axis=0, tiled=True),
    )
    summed = attn_rows + resid_rows.astype(jnp.float32)
    inverse_rms = lax.rsqrt(jnp.mean(summed * summed, axis=1) + small_eps)
    normed = summed * inverse_rms[:, None] * gain_cols.astype(jnp.float32)
    peak_abs = jnp.max(jnp.abs(normed), axis=1) + small_eps
    coded_rows = (normed / peak_abs[:, None]).astype(jnp.bfloat16)
    dispatched = jnp.dot(
        own_pick.astype(jnp.bfloat16), coded_rows, preferred_element_type=jnp.float32
    ).astype(jnp.bfloat16)
    slot_scale = jnp.dot(own_pick, peak_abs, precision=lax.Precision.HIGHEST)
    return (
        dispatched.reshape(experts_local, CAP, D),
        slot_scale.reshape(experts_local, CAP),
        slot_gate.reshape(experts_local, CAP),
    )


LANES = 128


def params(mebibytes=8):
    return pltpu.CompilerParams(vmem_limit_bytes=mebibytes * 1024 * 1024)


def whole(count):
    return [pl.BlockSpec(memory_space=pltpu.VMEM) for _ in range(count)]


def exchange_orders(width):
    falling = list(range(width - 1, 0, -1))
    return [falling[-1:] + falling[:-1], falling]


def from_crossing(value, steps):
    pairs = [(source, source ^ 2 ** steps[source % 2]) for source in range(lax.axis_size("kv"))]
    return lax.ppermute(value, "kv", pairs)


def distance(position, order):
    mask = 0
    for step, bit in enumerate(order):
        mask ^= (position >> step) % 2 * 2 ** (bit - 1)
    return mask


def join(*refs):
    out_ref, at = refs[-1], 0
    for ref in refs[:-1]:
        out_ref[at : at + ref.shape[0]] = ref[...]
        at += ref.shape[0]


def joined(parts):
    count = sum(part.shape[0] for part in parts)
    return pl.pallas_call(
        join,
        name="join",
        out_shape=jax.ShapeDtypeStruct((count,) + parts[0].shape[1:], parts[0].dtype),
        in_specs=whole(len(parts)),
        out_specs=whole(1)[0],
        compiler_params=params(),
    )(*parts)


def split_three(values):
    high = values.astype(jnp.bfloat16).astype(jnp.float32)
    middle = (values - high).astype(jnp.bfloat16).astype(jnp.float32)
    return high, middle, values - high - middle


def spread_stats(values):
    high, middle, low = split_three(values)
    lane = lax.broadcasted_iota(jnp.int32, values.shape, values.ndim - 1)
    axis = values.ndim - 1
    parts = jnp.where(lane < 64, pltpu.roll(middle, 32, axis), pltpu.roll(low, 64, axis))
    return jnp.where(lane < 32, high, parts).astype(jnp.bfloat16)


def gather_stats(tile):
    tile = tile.astype(jnp.float32)
    axis = tile.ndim - 1
    return tile + pltpu.roll(tile, LANES - 32, axis) + pltpu.roll(tile, LANES - 64, axis)


SEQS_AT_ONCE = 4


def attend(place_ref, lengths_ref, cache_ref, *refs):
    pieces, (keep_ref, send_ref, q_ref, o_ref) = refs[:-4], refs[-4:]
    half, seqs, payload = keep_ref.shape
    blocks = 2 * half
    heads = H // blocks
    entry, ctx_local = cache_ref.shape[1:]
    tiles = q_ref.shape[1]
    at = 0
    for ref in pieces:
        for block in range(ref.shape[0]):
            rows = ref[block].astype(jnp.float32)
            for h in range(heads):
                for t in range(tiles):
                    cols = slice(h * entry + t * LANES, h * entry + min((t + 1) * LANES, entry))
                    q_ref[h, t, at : at + seqs, : cols.stop - cols.start] = rows[:, cols]
            at += seqs
    first = place_ref[0] * ctx_local
    position = first + lax.broadcasted_iota(jnp.int32, (H, ctx_local), 1)
    lane = lax.broadcasted_iota(jnp.int32, (blocks, LANES), 1)

    def batch(number, carry):
        all_seqs = [number * SEQS_AT_ONCE + i for i in range(SEQS_AT_ONCE)]
        scores, tops, totals, weights, outs = [], [], [], [], []
        for seq in all_seqs:
            mine = pl.ds(seq, blocks, stride=seqs)
            query = jnp.concatenate(
                [
                    jnp.concatenate([q_ref[h, t, mine, :] for t in range(tiles)], axis=1)
                    for h in range(heads)
                ],
                axis=0,
            )[:, :entry].astype(jnp.bfloat16)
            scores.append(jnp.dot(query, cache_ref[seq], preferred_element_type=jnp.float32))
        for seq, score in zip(all_seqs, scores):
            valid = position < lengths_ref[seq]
            score = jnp.where(valid, score * score_scale, masked_score)
            top = jnp.max(score, axis=1, keepdims=True)
            weight = jnp.where(valid, jnp.exp(score - top), 0.0)
            tops.append(top)
            totals.append(jnp.sum(weight, axis=1, keepdims=True))
            weights.append(weight.astype(jnp.bfloat16))
        for seq, weight in zip(all_seqs, weights):
            outs.append(
                lax.dot_general(
                    weight,
                    cache_ref[seq, :LAT, :],
                    (((1,), (1,)), ((), ())),
                    preferred_element_type=jnp.float32,
                )
            )
        for seq, top, total, out in zip(all_seqs, tops, totals, outs):
            mine = pl.ds(seq, blocks, stride=seqs)
            stats = jnp.zeros((blocks, LANES), jnp.float32)
            for h in range(heads):
                part = slice(h * blocks, (h + 1) * blocks)
                for t in range(LAT // LANES):
                    o_ref[h * (LAT // LANES) + t, mine, :] = out[part, t * LANES : (t + 1) * LANES]
                stats = jnp.where(lane == 2 * h, top[part], stats)
                stats = jnp.where(lane == 2 * h + 1, total[part], stats)
            o_ref[heads * LAT // LANES, mine, :] = stats
        return carry

    lax.fori_loop(0, seqs // SEQS_AT_ONCE, batch, 0)
    chip, north = place_ref[0] // 2, place_ref[0] % 2 == 1
    orders = exchange_orders(blocks.bit_length() - 1)
    last = heads * LAT // LANES
    for block in range(half):
        even, odd = (distance(block, order) for order in orders)
        to = chip ^ jnp.where(north, odd, even)
        at = block * seqs
        for t in range(last + 1):
            keep_ref[to, :, t * LANES : (t + 1) * LANES] = o_ref[t, at : at + seqs, :]
        to = chip ^ jnp.where(north, even, odd)
        at = (half + block) * seqs
        for t in range(last):
            cols = slice(t * LANES, (t + 1) * LANES)
            send_ref[to, :, cols] = o_ref[t, at : at + seqs, :].astype(jnp.bfloat16)
        send_ref[to, :, heads * LAT :] = spread_stats(o_ref[last, at : at + seqs, :])


def merge_pair(keep_ref, got_ref, out_ref):
    half, seqs, width = keep_ref.shape
    heads = (width - LANES) // LAT
    lane = lax.broadcasted_iota(jnp.int32, (seqs, LANES), 1)

    def step(block, carry):
        mine = keep_ref[block, :, heads * LAT :]
        theirs = gather_stats(got_ref[block, :, heads * LAT :])
        stats = jnp.zeros((seqs, LANES), jnp.float32)
        for h in range(heads):
            top_a, top_b = mine[:, 2 * h : 2 * h + 1], theirs[:, 2 * h : 2 * h + 1]
            sum_a, sum_b = mine[:, 2 * h + 1 : 2 * h + 2], theirs[:, 2 * h + 1 : 2 * h + 2]
            top = jnp.maximum(top_a, top_b)
            scale_a, scale_b = jnp.exp(top_a - top), jnp.exp(top_b - top)
            total = sum_a * scale_a + sum_b * scale_b
            cols = slice(h * LAT, (h + 1) * LAT)
            out_ref[block, :, cols] = (
                keep_ref[block, :, cols] * scale_a
                + got_ref[block, :, cols].astype(jnp.float32) * scale_b
            ).astype(jnp.bfloat16)
            stats = jnp.where(lane == 2 * h, top, stats)
            stats = jnp.where(lane == 2 * h + 1, total, stats)
        out_ref[block, :, heads * LAT :] = spread_stats(stats)
        return carry

    lax.fori_loop(0, half, step, 0, unroll=2)


def project(place_ref, got_ref, up_ref, proj_ref, keep_ref, send_ref):
    half, seqs, width = got_ref.shape
    heads = (width - LANES) // LAT
    stats = [gather_stats(got_ref[c, :, heads * LAT :]) for c in range(half)]
    values = []
    for h in range(heads):
        tops = [s[:, 2 * h : 2 * h + 1] for s in stats]
        top = tops[0]
        for t in tops[1:]:
            top = jnp.maximum(top, t)
        scales = [jnp.exp(t - top) for t in tops]
        total = sum(s[:, 2 * h + 1 : 2 * h + 2] * x for s, x in zip(stats, scales))
        merged = sum(
            got_ref[c, :, h * LAT : (h + 1) * LAT].astype(jnp.float32) * scales[c]
            for c in range(half)
        )
        merged = merged / total
        high = merged.astype(jnp.bfloat16)
        low = (merged - high.astype(jnp.float32)).astype(jnp.bfloat16)
        up = up_ref[h * LAT : (h + 1) * LAT, :]
        value = jnp.dot(high, up, preferred_element_type=jnp.float32)
        value = value + jnp.dot(low, up, preferred_element_type=jnp.float32)
        values.append(value.astype(jnp.bfloat16))
    rows = jnp.concatenate(values, axis=1)
    cols = proj_ref.shape[1] // half
    part = cols // 2
    pad = send_ref.shape[2] - part
    north = place_ref[0] % 2 == 1
    zeros = jnp.zeros((seqs, pad), jnp.float32)
    for c in range(half):
        out = jnp.dot(
            rows, proj_ref[:, c * cols : (c + 1) * cols], preferred_element_type=jnp.float32
        )
        even = jnp.concatenate([out[:, :part], zeros], axis=1)
        odd = jnp.concatenate([out[:, part:], zeros], axis=1)
        keep_ref[c] = jnp.where(north, odd, even)
        send_ref[c] = jnp.where(north, even, odd).astype(jnp.bfloat16)


def normalise(got_ref, residual_ref, gain_ref, out_ref):
    half, seqs, width = got_ref.shape
    part = residual_ref.shape[1]
    total = got_ref[0].astype(jnp.float32)
    for c in range(1, half):
        total = total + got_ref[c].astype(jnp.float32)
    summed = total[:, :part] + residual_ref[...].astype(jnp.float32)
    squares = jnp.sum(summed * summed, axis=1, keepdims=True)
    gained = summed * gain_ref[...].astype(jnp.float32)
    peak = jnp.max(jnp.abs(gained), axis=1, keepdims=True)
    pad = width - part
    lane = lax.broadcasted_iota(jnp.int32, (seqs, pad), 1)
    stats = jnp.zeros((seqs, pad), jnp.float32)
    for at, piece in enumerate(split_three(squares) + split_three(peak)):
        stats = jnp.where(lane == at, piece, stats)
    row = jnp.concatenate([gained, stats], axis=1).astype(jnp.bfloat16)
    for c in range(half):
        out_ref[c] = row


def route(place_ref, ids_ref, gates_ref, pick_ref, gate_ref):
    count, seqs = ids_ref.shape
    experts = gate_ref.shape[1]
    expert = place_ref[0] * experts + lax.broadcasted_iota(jnp.int32, (experts, seqs), 0)
    named = jnp.zeros((experts, seqs), jnp.float32)
    gates = jnp.zeros((experts, seqs), jnp.float32)
    for k in range(count):
        same = ids_ref[k : k + 1, :] == expert
        named = jnp.where(same, 1.0, named)
        gates = jnp.where(same, gates_ref[k : k + 1, :], gates)
    earlier = lax.broadcasted_iota(jnp.int32, (seqs, seqs), 0)
    later = lax.broadcasted_iota(jnp.int32, (seqs, seqs), 1)
    before = jnp.where(earlier < later, 1.0, 0.0).astype(jnp.bfloat16)
    slot = jnp.dot(named.astype(jnp.bfloat16), before, preferred_element_type=jnp.float32)
    picks, rows = [], []
    for c in range(CAP):
        pick = jnp.where(slot == c, named, 0.0)
        picks.append(pick)
        chosen = jnp.sum(pick * gates, axis=1, keepdims=True)
        rows.append(jnp.transpose(jnp.broadcast_to(chosen, (experts, LANES)), (1, 0))[:1])
    gate_ref[...] = jnp.concatenate(rows, axis=0)
    pick_ref[...] = jnp.concatenate(picks, axis=0)


def finish(place_ref, own_ref, other_ref, pick_ref, out_ref, scale_ref):
    half, seqs, width = own_ref.shape
    cols = out_ref.shape[2] // half
    part = cols // 2
    north = place_ref[0] % 2 == 1
    squares = jnp.zeros((seqs, 1), jnp.float32)
    peak = jnp.zeros((seqs, 1), jnp.float32)
    for ref in (own_ref, other_ref):
        for c in range(half):
            stats = ref[c, :, part:].astype(jnp.float32)
            squares = squares + stats[:, 0:1] + stats[:, 1:2] + stats[:, 2:3]
            peak = jnp.maximum(peak, stats[:, 3:4] + stats[:, 4:5] + stats[:, 5:6])
    inverse_rms = lax.rsqrt(squares / (cols * half) + small_eps)
    peak = peak * inverse_rms + small_eps
    factor = inverse_rms / peak
    experts = scale_ref.shape[1]
    peaks = jnp.transpose(jnp.broadcast_to(peak, (seqs, LANES)), (1, 0))[:1]
    scales = jnp.sum(pick_ref[...] * peaks, axis=1, keepdims=True)
    scales = jnp.transpose(jnp.broadcast_to(scales, (CAP * experts, LANES)), (1, 0))[:1]
    for c in range(CAP):
        scale_ref[c : c + 1, :] = scales[:, c * experts : (c + 1) * experts]
    picks = [pick_ref[c * experts : (c + 1) * experts, :] for c in range(CAP)]
    pick = jnp.concatenate([p[:, None, :] for p in picks], axis=1)
    pick = pick.reshape(CAP * experts, seqs).astype(jnp.bfloat16)
    for c in range(half):
        own, other = own_ref[c, :, :part], other_ref[c, :, :part]
        pair = jnp.concatenate(
            [jnp.where(north, other, own), jnp.where(north, own, other)], axis=1
        )
        coded = (pair.astype(jnp.float32) * factor).astype(jnp.bfloat16)
        rows = jnp.dot(pick, coded, preferred_element_type=jnp.float32).astype(jnp.bfloat16)
        out_ref[:, :, c * cols : (c + 1) * cols] = rows.reshape(experts, CAP, cols)


def whole_heads(
    queries,
    latent_cache,
    context_lengths,
    value_up,
    out_proj,
    residual,
    norm_gain,
    expert_ids,
    gate_weights,
):
    kv_count = lax.axis_size("kv")
    shard_index = lax.axis_index("kv")
    half = kv_count // 2
    seq_count, width = queries.shape
    place = shard_index.reshape(1).astype(jnp.int32)
    chips = [[2 * c + core for c in range(half)] for core in range(2)]
    smem = pl.BlockSpec(memory_space=pltpu.SMEM)

    def across_chips(value):
        return lax.all_to_all(value, "kv", 0, 0, axis_index_groups=chips, tiled=True)

    orders = exchange_orders(kv_count.bit_length() - 1)
    pieces = [queries.reshape(1, seq_count, width)]
    others = [from_partner(pieces[0], "kv", 0)]
    for steps in zip(*orders):
        sent = pieces[0] if len(pieces) == 1 else joined(pieces)
        pieces.append(from_crossing(sent, steps))
        others.append(from_partner(pieces[-1], "kv", 0))
    pieces = pieces + others

    payload = H * LAT // kv_count + LANES
    block = (half, seq_count, payload)
    entry = LAT + ROPE
    tiles = (entry + LANES - 1) // LANES
    rows = kv_count * seq_count
    keep, send = pl.pallas_call(
        attend,
        name="attend",
        out_shape=(
            jax.ShapeDtypeStruct(block, jnp.float32),
            jax.ShapeDtypeStruct(block, jnp.bfloat16),
        ),
        in_specs=[smem, smem] + whole(1 + len(pieces)),
        out_specs=tuple(whole(2)),
        scratch_shapes=[
            pltpu.VMEM((H // kv_count, tiles, rows, LANES), jnp.float32),
            pltpu.VMEM((payload // LANES, rows, LANES), jnp.float32),
        ],
        compiler_params=params(14),
    )(place, context_lengths, jnp.swapaxes(latent_cache, 1, 2), *pieces)
    got = from_partner(send, "kv", 0)
    merged = pl.pallas_call(
        merge_pair,
        name="merge_pair",
        out_shape=jax.ShapeDtypeStruct(block, jnp.bfloat16),
        in_specs=whole(2),
        out_specs=whole(1)[0],
        compiler_params=params(),
    )(keep, got)
    got = across_chips(merged)

    part = out_proj.shape[1] // kv_count
    padded = (part + 6 + LANES - 1) // LANES * LANES
    strip = (half, seq_count, padded)
    keep, send = pl.pallas_call(
        project,
        name="project",
        out_shape=(
            jax.ShapeDtypeStruct(strip, jnp.float32),
            jax.ShapeDtypeStruct(strip, jnp.bfloat16),
        ),
        in_specs=[smem] + whole(3),
        out_specs=tuple(whole(2)),
        compiler_params=params(),
    )(place, got, value_up, out_proj)
    got = from_partner(send, "kv", 0)
    got = across_chips((keep + got.astype(jnp.float32)).astype(jnp.bfloat16))
    copies = pl.pallas_call(
        normalise,
        name="normalise",
        out_shape=jax.ShapeDtypeStruct(strip, jnp.bfloat16),
        in_specs=whole(3),
        out_specs=whole(1)[0],
        compiler_params=params(),
    )(got, residual, norm_gain.reshape(1, part))
    own = across_chips(copies)
    other = from_partner(own, "kv", 0)

    experts_local = EXPERTS // kv_count
    pick, slot_gate = pl.pallas_call(
        route,
        name="route",
        out_shape=(
            jax.ShapeDtypeStruct((CAP * experts_local, seq_count), jnp.float32),
            jax.ShapeDtypeStruct((CAP, experts_local), jnp.float32),
        ),
        in_specs=[smem] + whole(2),
        out_specs=tuple(whole(2)),
        compiler_params=params(),
    )(place, expert_ids.T, gate_weights.T)
    dispatched, slot_scale = pl.pallas_call(
        finish,
        name="finish",
        out_shape=(
            jax.ShapeDtypeStruct((experts_local, CAP, out_proj.shape[1]), jnp.bfloat16),
            jax.ShapeDtypeStruct((CAP, experts_local), jnp.float32),
        ),
        in_specs=[smem] + whole(3),
        out_specs=tuple(whole(2)),
        compiler_params=params(),
    )(place, own, other, pick)
    return dispatched, slot_scale.T, slot_gate.T


def per_device(*args):
    if lax.axis_size("kv") > H:
        return split_heads(*args)
    return whole_heads(*args)


def solution(mesh):
    in_specs = (
        P("groups", "kv"),
        P("groups", "kv", None),
        P("groups"),
        P("kv", None),
        P("kv", None),
        P("groups", "kv"),
        P("kv"),
        P("groups", None),
        P("groups", None),
    )
    out_specs = (
        P(("groups", "kv"), None, None),
        P(("groups", "kv"), None),
        P(("groups", "kv"), None),
    )
    return jax.shard_map(
        per_device, mesh=mesh, in_specs=in_specs, out_specs=out_specs, check_vma=False
    )
```

```python
import jax
import jax.numpy as jnp
from jax import lax
from jax.experimental import pallas as pl
from jax.experimental.pallas import tpu as pltpu
from jax.sharding import PartitionSpec as P

H = 32
LAT = 512
ROPE = 64
VD = 128
D = 7168
EXPERTS = 256
TOPK = 8
CAP = 2


score_scale = 192.0 ** (-0.5)
masked_score = -1e30
small_eps = 1e-06


def from_partner(value, axis, bit):
    mask = 2**bit
    pairs = [(source, source ^ mask) for source in range(lax.axis_size(axis))]
    return lax.ppermute(value, axis, pairs)


def slot_targets(expert_ids):
    flat_ids = expert_ids.reshape(-1)
    order_index = jnp.arange(flat_ids.shape[0], dtype=jnp.int32)
    same_before = (flat_ids[:, None] == flat_ids[None, :]) & (
        order_index[None, :] < order_index[:, None]
    )
    rank_within = jnp.sum(same_before.astype(jnp.int32), axis=1)
    return flat_ids * CAP + rank_within


def slot_match(targets, first_slot, slot_count):
    slot_index = first_slot + jnp.arange(slot_count, dtype=jnp.int32)
    return (slot_index[:, None] == targets[None, :]).astype(jnp.float32)


def token_picker(matches, seq_count):
    return jnp.sum(matches.reshape(matches.shape[0], seq_count, TOPK), axis=2)


def split_heads(
    queries,
    latent_cache,
    context_lengths,
    value_up,
    out_proj,
    residual,
    norm_gain,
    expert_ids,
    gate_weights,
):
    kv_count = lax.axis_size("kv")
    shard_index = lax.axis_index("kv")
    seq_count = queries.shape[0]
    query_rows = lax.all_gather(queries, "kv", axis=1, tiled=True).reshape(seq_count, H, LAT + ROPE)
    ctx_local = latent_cache.shape[1]
    scores = (
        jnp.einsum("shq,scq->shc", query_rows, latent_cache, preferred_element_type=jnp.float32)
        * score_scale
    )
    position = shard_index * ctx_local + jnp.arange(ctx_local, dtype=jnp.int32)
    valid_mask = (position[None, :] < context_lengths[:, None])[:, None, :]
    scores = jnp.where(valid_mask, scores, masked_score)
    local_max = jnp.max(scores, axis=2)
    weights = jnp.where(valid_mask, jnp.exp(scores - local_max[:, :, None]), 0.0)
    local_total = jnp.sum(weights, axis=2)
    local_out = jnp.einsum(
        "shc,scl->shl",
        weights.astype(jnp.bfloat16),
        latent_cache[:, :, :LAT],
        preferred_element_type=jnp.float32,
    )
    out_rows = out_proj.shape[0]
    col_count = H * LAT // kv_count
    segment = min(col_count, LAT)
    head_count = col_count // segment
    head_start = shard_index * col_count // LAT
    global_max = lax.pmax(local_max, "kv")
    scaling = jnp.exp(local_max - global_max)
    weight_total = lax.psum(local_total * scaling, "kv")
    scaled = (local_out * scaling[:, :, None]).reshape(seq_count, H * LAT)
    merged_sum = lax.psum_scatter(scaled, "kv", scatter_dimension=1, tiled=True).reshape(
        seq_count, head_count, segment
    )
    own_total = lax.dynamic_slice_in_dim(weight_total, head_start, head_count, 1)
    merged = merged_sum / own_total[:, :, None]
    projector = value_up.reshape(head_count, segment, VD).astype(jnp.float32)
    value_part = jnp.einsum("shl,hlv->shv", merged, projector, precision=lax.Precision.HIGHEST)
    holders = kv_count // H if kv_count > H else 1
    for bit in range(holders.bit_length() - 1):
        value_part = value_part + from_partner(value_part, "kv", bit)
    value_rows = value_part.astype(jnp.bfloat16).reshape(seq_count, head_count * VD)
    if holders > 1:
        value_rows = lax.dynamic_slice_in_dim(
            value_rows, shard_index % holders * out_rows, out_rows, 1
        )
    partial_out = jnp.dot(value_rows, out_proj, preferred_element_type=jnp.float32)
    experts_local = EXPERTS // kv_count
    slot_count = experts_local * CAP
    targets = slot_targets(expert_ids)
    own_match = slot_match(targets, shard_index * slot_count, slot_count)
    own_pick = token_picker(own_match, seq_count)
    slot_gate = jnp.dot(own_match, gate_weights.reshape(-1), precision=lax.Precision.HIGHEST)
    attn_rows = lax.psum(partial_out, "kv")
    resid_rows, gain_cols = (
        lax.all_gather(residual, "kv", axis=1, tiled=True),
        lax.all_gather(norm_gain, "kv", axis=0, tiled=True),
    )
    summed = attn_rows + resid_rows.astype(jnp.float32)
    inverse_rms = lax.rsqrt(jnp.mean(summed * summed, axis=1) + small_eps)
    normed = summed * inverse_rms[:, None] * gain_cols.astype(jnp.float32)
    peak_abs = jnp.max(jnp.abs(normed), axis=1) + small_eps
    coded_rows = (normed / peak_abs[:, None]).astype(jnp.bfloat16)
    dispatched = jnp.dot(
        own_pick.astype(jnp.bfloat16), coded_rows, preferred_element_type=jnp.float32
    ).astype(jnp.bfloat16)
    slot_scale = jnp.dot(own_pick, peak_abs, precision=lax.Precision.HIGHEST)
    return (
        dispatched.reshape(experts_local, CAP, D),
        slot_scale.reshape(experts_local, CAP),
        slot_gate.reshape(experts_local, CAP),
    )


LANES = 128


def params(mebibytes=8):
    return pltpu.CompilerParams(vmem_limit_bytes=mebibytes * 1024 * 1024)


def whole(count):
    return [pl.BlockSpec(memory_space=pltpu.VMEM) for _ in range(count)]


def gather_orders(width):
    falling = list(range(width - 1, 0, -1))
    return [falling[-1:] + falling[:-1], falling]


def scatter_orders(width):
    rising = list(range(1, width))
    return [rising, rising[1:] + rising[:1]]


def from_crossing(value, steps):
    pairs = [(source, source ^ 2 ** steps[source % 2]) for source in range(lax.axis_size("kv"))]
    return lax.ppermute(value, "kv", pairs)


def distance(position, order):
    mask = 0
    for step, bit in enumerate(order):
        mask ^= (position >> step) % 2 * 2 ** (bit - 1)
    return mask


def landing(position, gather, scatter):
    mask = distance(position, gather)
    places = range(2 ** len(scatter))
    return next(place for place in places if distance(place, scatter[::-1]) == mask)


def join(*refs):
    out_ref, at = refs[-1], 0
    for ref in refs[:-1]:
        out_ref[at : at + ref.shape[0]] = ref[...]
        at += ref.shape[0]


def joined(parts):
    count = sum(part.shape[0] for part in parts)
    return pl.pallas_call(
        join,
        name="join",
        out_shape=jax.ShapeDtypeStruct((count,) + parts[0].shape[1:], parts[0].dtype),
        in_specs=whole(len(parts)),
        out_specs=whole(1)[0],
        compiler_params=params(),
    )(*parts)


def split_three(values):
    high = values.astype(jnp.bfloat16).astype(jnp.float32)
    middle = (values - high).astype(jnp.bfloat16).astype(jnp.float32)
    return high, middle, values - high - middle


def spread_stats(values):
    high, middle, low = split_three(values)
    lane = lax.broadcasted_iota(jnp.int32, values.shape, values.ndim - 1)
    axis = values.ndim - 1
    parts = jnp.where(lane < 64, pltpu.roll(middle, 32, axis), pltpu.roll(low, 64, axis))
    return jnp.where(lane < 32, high, parts).astype(jnp.bfloat16)


def gather_stats(tile):
    tile = tile.astype(jnp.float32)
    axis = tile.ndim - 1
    return tile + pltpu.roll(tile, LANES - 32, axis) + pltpu.roll(tile, LANES - 64, axis)


SEQS_AT_ONCE = 8


def attend(place_ref, lengths_hbm, cache_hbm, *refs):
    pieces, refs = refs[:-8], refs[-8:]
    keep_ref, send_ref, q_ref, o_ref, lengths_ref, cache_ref, length_done, cache_done = refs
    length_copy = pltpu.make_async_copy(lengths_hbm, lengths_ref, length_done)
    length_copy.start()

    def cache_copy(number):
        some = pl.ds(number * SEQS_AT_ONCE, SEQS_AT_ONCE)
        return pltpu.make_async_copy(cache_hbm.at[some], cache_ref.at[some], cache_done.at[number])

    for number in range(cache_done.shape[0]):
        cache_copy(number).start()
    half, seqs, payload = keep_ref.shape
    blocks = 2 * half
    heads = H // blocks
    entry, ctx_local = cache_ref.shape[1:]
    tiles = q_ref.shape[1]
    at = 0
    for ref in pieces:
        for block in range(ref.shape[0]):
            rows = ref[block].astype(jnp.float32)
            for h in range(heads):
                for t in range(tiles):
                    cols = slice(h * entry + t * LANES, h * entry + min((t + 1) * LANES, entry))
                    q_ref[h, t, at : at + seqs, : cols.stop - cols.start] = rows[:, cols]
            at += seqs
    first = place_ref[0] * ctx_local
    position = first + lax.broadcasted_iota(jnp.int32, (H, ctx_local), 1)
    lane = lax.broadcasted_iota(jnp.int32, (blocks, LANES), 1)
    length_copy.wait()

    def batch(number, carry):
        cache_copy(number).wait()
        all_seqs = [number * SEQS_AT_ONCE + i for i in range(SEQS_AT_ONCE)]
        scores, tops, totals, weights, outs = [], [], [], [], []
        for seq in all_seqs:
            mine = pl.ds(seq, blocks, stride=seqs)
            query = jnp.concatenate(
                [
                    jnp.concatenate([q_ref[h, t, mine, :] for t in range(tiles)], axis=1)
                    for h in range(heads)
                ],
                axis=0,
            )[:, :entry].astype(jnp.bfloat16)
            scores.append(jnp.dot(query, cache_ref[seq], preferred_element_type=jnp.float32))
        for seq, score in zip(all_seqs, scores):
            valid = position < lengths_ref[seq]
            score = jnp.where(valid, score * score_scale, masked_score)
            top = jnp.max(score, axis=1, keepdims=True)
            weight = jnp.where(valid, jnp.exp(score - top), 0.0)
            tops.append(top)
            totals.append(jnp.sum(weight, axis=1, keepdims=True))
            weights.append(weight.astype(jnp.bfloat16))
        for seq, weight in zip(all_seqs, weights):
            outs.append(
                lax.dot_general(
                    weight,
                    cache_ref[seq, :LAT, :],
                    (((1,), (1,)), ((), ())),
                    preferred_element_type=jnp.float32,
                )
            )
        for seq, top, total, out in zip(all_seqs, tops, totals, outs):
            mine = pl.ds(seq, blocks, stride=seqs)
            stats = jnp.zeros((blocks, LANES), jnp.float32)
            for h in range(heads):
                part = slice(h * blocks, (h + 1) * blocks)
                for t in range(LAT // LANES):
                    o_ref[h * (LAT // LANES) + t, mine, :] = out[part, t * LANES : (t + 1) * LANES]
                stats = jnp.where(lane == 2 * h, top[part], stats)
                stats = jnp.where(lane == 2 * h + 1, total[part], stats)
            o_ref[heads * LAT // LANES, mine, :] = stats
        return carry

    lax.fori_loop(0, seqs // SEQS_AT_ONCE, batch, 0)
    north = place_ref[0] % 2 == 1
    width = blocks.bit_length() - 1
    gathers, scatters = gather_orders(width), scatter_orders(width)
    last = heads * LAT // LANES
    for block in range(half):
        even = landing(block, gathers[0], scatters[0])
        odd = landing(block, gathers[1], scatters[1])
        to = jnp.where(north, odd, even)
        at = block * seqs
        for t in range(last + 1):
            keep_ref[to, :, t * LANES : (t + 1) * LANES] = o_ref[t, at : at + seqs, :]
        even = landing(block, gathers[1], scatters[1])
        odd = landing(block, gathers[0], scatters[0])
        to = jnp.where(north, odd, even)
        at = (half + block) * seqs
        for t in range(last):
            cols = slice(t * LANES, (t + 1) * LANES)
            send_ref[to, :, cols] = o_ref[t, at : at + seqs, :].astype(jnp.bfloat16)
        send_ref[to, :, heads * LAT :] = spread_stats(o_ref[last, at : at + seqs, :])


def merge_block(keep_ref, got_ref, block, heads):
    mine = keep_ref[block, :, heads * LAT :]
    theirs = gather_stats(got_ref[block, :, heads * LAT :])
    lane = lax.broadcasted_iota(jnp.int32, mine.shape, 1)
    stats, parts = jnp.zeros(mine.shape, jnp.float32), []
    for h in range(heads):
        top_a, top_b = mine[:, 2 * h : 2 * h + 1], theirs[:, 2 * h : 2 * h + 1]
        sum_a, sum_b = mine[:, 2 * h + 1 : 2 * h + 2], theirs[:, 2 * h + 1 : 2 * h + 2]
        top = jnp.maximum(top_a, top_b)
        scale_a, scale_b = jnp.exp(top_a - top), jnp.exp(top_b - top)
        cols = slice(h * LAT, (h + 1) * LAT)
        parts.append(
            keep_ref[block, :, cols] * scale_a
            + got_ref[block, :, cols].astype(jnp.float32) * scale_b
        )
        stats = jnp.where(lane == 2 * h, top, stats)
        stats = jnp.where(lane == 2 * h + 1, sum_a * scale_a + sum_b * scale_b, stats)
    return parts, stats


def merge_kept(keep_ref, got_ref, out_ref):
    heads = (out_ref.shape[2] - LANES) // LAT
    for block in range(out_ref.shape[0]):
        parts, stats = merge_block(keep_ref, got_ref, block, heads)
        for h, part in enumerate(parts):
            out_ref[block, :, h * LAT : (h + 1) * LAT] = part
        out_ref[block, :, heads * LAT :] = stats


def merge_sent(keep_ref, got_ref, out_ref):
    heads = (out_ref.shape[2] - LANES) // LAT
    for block in range(out_ref.shape[0]):
        parts, stats = merge_block(keep_ref, got_ref, out_ref.shape[0] + block, heads)
        for h, part in enumerate(parts):
            out_ref[block, :, h * LAT : (h + 1) * LAT] = part.astype(jnp.bfloat16)
        out_ref[block, :, heads * LAT :] = spread_stats(stats)


def add_pair(keep_ref, got_ref, out_ref):
    for block in range(keep_ref.shape[0]):
        total = keep_ref[block] + got_ref[block].astype(jnp.float32)
        out_ref[block] = total.astype(jnp.bfloat16)


def project(place_ref, mine_ref, got_ref, up_ref, proj_ref, keep_ref, send_ref):
    half, seqs, _ = keep_ref.shape
    heads = (mine_ref.shape[2] - LANES) // LAT
    parts, stats = merge_block(mine_ref, got_ref, 0, heads)
    values = []
    for h, part in enumerate(parts):
        merged = part / stats[:, 2 * h + 1 : 2 * h + 2]
        high = merged.astype(jnp.bfloat16)
        low = (merged - high.astype(jnp.float32)).astype(jnp.bfloat16)
        up = up_ref[h * LAT : (h + 1) * LAT, :]
        value = jnp.dot(high, up, preferred_element_type=jnp.float32)
        value = value + jnp.dot(low, up, preferred_element_type=jnp.float32)
        values.append(value.astype(jnp.bfloat16))
    rows = jnp.concatenate(values, axis=1)
    cols = proj_ref.shape[1] // half
    part = cols // 2
    pad = send_ref.shape[2] - part
    north = place_ref[0] % 2 == 1
    zeros = jnp.zeros((seqs, pad), jnp.float32)
    for c in range(half):
        out = jnp.dot(
            rows, proj_ref[:, c * cols : (c + 1) * cols], preferred_element_type=jnp.float32
        )
        even = jnp.concatenate([out[:, :part], zeros], axis=1)
        odd = jnp.concatenate([out[:, part:], zeros], axis=1)
        keep_ref[c] = jnp.where(north, odd, even)
        send_ref[c] = jnp.where(north, even, odd).astype(jnp.bfloat16)


def normalise(got_ref, residual_ref, gain_ref, out_ref):
    half, seqs, width = got_ref.shape
    part = residual_ref.shape[1]
    total = got_ref[0].astype(jnp.float32)
    for c in range(1, half):
        total = total + got_ref[c].astype(jnp.float32)
    summed = total[:, :part] + residual_ref[...].astype(jnp.float32)
    squares = jnp.sum(summed * summed, axis=1, keepdims=True)
    gained = summed * gain_ref[...].astype(jnp.float32)
    peak = jnp.max(jnp.abs(gained), axis=1, keepdims=True)
    pad = width - part
    lane = lax.broadcasted_iota(jnp.int32, (seqs, pad), 1)
    stats = jnp.zeros((seqs, pad), jnp.float32)
    for at, piece in enumerate(split_three(squares) + split_three(peak)):
        stats = jnp.where(lane == at, piece, stats)
    row = jnp.concatenate([gained, stats], axis=1).astype(jnp.bfloat16)
    for c in range(half):
        out_ref[c] = row


def route(place_ref, ids_ref, gates_ref, pick_ref, gate_ref):
    count, seqs = ids_ref.shape
    experts = gate_ref.shape[1]
    expert = place_ref[0] * experts + lax.broadcasted_iota(jnp.int32, (experts, seqs), 0)
    named = jnp.zeros((experts, seqs), jnp.float32)
    gates = jnp.zeros((experts, seqs), jnp.float32)
    for k in range(count):
        same = ids_ref[k : k + 1, :] == expert
        named = jnp.where(same, 1.0, named)
        gates = jnp.where(same, gates_ref[k : k + 1, :], gates)
    earlier = lax.broadcasted_iota(jnp.int32, (seqs, seqs), 0)
    later = lax.broadcasted_iota(jnp.int32, (seqs, seqs), 1)
    before = jnp.where(earlier < later, 1.0, 0.0).astype(jnp.bfloat16)
    slot = jnp.dot(named.astype(jnp.bfloat16), before, preferred_element_type=jnp.float32)
    picks, rows = [], []
    for c in range(CAP):
        pick = jnp.where(slot == c, named, 0.0)
        picks.append(pick)
        chosen = jnp.sum(pick * gates, axis=1, keepdims=True)
        rows.append(jnp.transpose(jnp.broadcast_to(chosen, (experts, LANES)), (1, 0))[:1])
    gate_ref[...] = jnp.concatenate(rows, axis=0)
    pick_ref[...] = jnp.concatenate(picks, axis=0)


def finish(place_ref, own_ref, other_ref, pick_ref, out_ref, scale_ref):
    half, seqs, width = own_ref.shape
    cols = out_ref.shape[2] // half
    part = cols // 2
    north = place_ref[0] % 2 == 1
    squares = jnp.zeros((seqs, 1), jnp.float32)
    peak = jnp.zeros((seqs, 1), jnp.float32)
    for ref in (own_ref, other_ref):
        for c in range(half):
            stats = ref[c, :, part:].astype(jnp.float32)
            squares = squares + stats[:, 0:1] + stats[:, 1:2] + stats[:, 2:3]
            peak = jnp.maximum(peak, stats[:, 3:4] + stats[:, 4:5] + stats[:, 5:6])
    inverse_rms = lax.rsqrt(squares / (cols * half) + small_eps)
    peak = peak * inverse_rms + small_eps
    factor = inverse_rms / peak
    experts = scale_ref.shape[1]
    peaks = jnp.transpose(jnp.broadcast_to(peak, (seqs, LANES)), (1, 0))[:1]
    scales = jnp.sum(pick_ref[...] * peaks, axis=1, keepdims=True)
    scales = jnp.transpose(jnp.broadcast_to(scales, (CAP * experts, LANES)), (1, 0))[:1]
    for c in range(CAP):
        scale_ref[c : c + 1, :] = scales[:, c * experts : (c + 1) * experts]
    picks = [pick_ref[c * experts : (c + 1) * experts, :] for c in range(CAP)]
    pick = jnp.concatenate([p[:, None, :] for p in picks], axis=1)
    pick = pick.reshape(CAP * experts, seqs).astype(jnp.bfloat16)
    for c in range(half):
        own, other = own_ref[c, :, :part], other_ref[c, :, :part]
        pair = jnp.concatenate(
            [jnp.where(north, other, own), jnp.where(north, own, other)], axis=1
        )
        coded = (pair.astype(jnp.float32) * factor).astype(jnp.bfloat16)
        rows = jnp.dot(pick, coded, preferred_element_type=jnp.float32).astype(jnp.bfloat16)
        out_ref[:, :, c * cols : (c + 1) * cols] = rows.reshape(experts, CAP, cols)


def whole_heads(
    queries,
    latent_cache,
    context_lengths,
    value_up,
    out_proj,
    residual,
    norm_gain,
    expert_ids,
    gate_weights,
):
    kv_count = lax.axis_size("kv")
    shard_index = lax.axis_index("kv")
    half = kv_count // 2
    seq_count, width = queries.shape
    place = shard_index.reshape(1).astype(jnp.int32)
    chips = [[2 * c + core for c in range(half)] for core in range(2)]
    smem = pl.BlockSpec(memory_space=pltpu.SMEM)
    hbm = pl.BlockSpec(memory_space=pltpu.HBM)

    def across_chips(value):
        return lax.all_to_all(value, "kv", 0, 0, axis_index_groups=chips, tiled=True)

    bits = kv_count.bit_length() - 1
    first = queries.reshape(1, seq_count, width)
    pieces = [joined([first])]
    others = [from_partner(first, "kv", 0)]
    for steps in zip(*gather_orders(bits)):
        sent = first if len(pieces) == 1 else joined(pieces)
        pieces.append(from_crossing(sent, steps))
        others.append(from_partner(pieces[-1], "kv", 0))
    pieces = pieces + others

    payload = H * LAT // kv_count + LANES
    block = (half, seq_count, payload)
    entry = LAT + ROPE
    tiles = (entry + LANES - 1) // LANES
    rows = kv_count * seq_count
    keep, send = pl.pallas_call(
        attend,
        name="attend",
        out_shape=(
            jax.ShapeDtypeStruct(block, jnp.float32),
            jax.ShapeDtypeStruct(block, jnp.bfloat16),
        ),
        in_specs=[smem, hbm, hbm] + whole(len(pieces)),
        out_specs=tuple(whole(2)),
        scratch_shapes=[
            pltpu.VMEM((H // kv_count, tiles, rows, LANES), jnp.float32),
            pltpu.VMEM((payload // LANES, rows, LANES), jnp.float32),
            pltpu.SMEM((seq_count,), jnp.int32),
            pltpu.VMEM((seq_count, entry, latent_cache.shape[1]), latent_cache.dtype),
            pltpu.SemaphoreType.DMA,
            pltpu.SemaphoreType.DMA((seq_count // SEQS_AT_ONCE,)),
        ],
        compiler_params=params(20),
    )(
        place,
        pltpu.with_memory_space_constraint(context_lengths, pltpu.HBM),
        pltpu.with_memory_space_constraint(jnp.swapaxes(latent_cache, 1, 2), pltpu.HBM),
        *pieces,
    )
    got = from_partner(send, "kv", 0)
    for steps in zip(*scatter_orders(bits)):
        count = keep.shape[0] // 2

        def merged(kernel, dtype):
            return pl.pallas_call(
                kernel,
                name=kernel.__name__,
                out_shape=jax.ShapeDtypeStruct((count,) + keep.shape[1:], dtype),
                in_specs=whole(2),
                out_specs=whole(1)[0],
                compiler_params=params(),
            )(keep, got)

        send, keep = merged(merge_sent, jnp.bfloat16), merged(merge_kept, jnp.float32)
        got = from_crossing(send, steps)

    part = out_proj.shape[1] // kv_count
    padded = (part + 6 + LANES - 1) // LANES * LANES
    strip = (half, seq_count, padded)
    keep, send = pl.pallas_call(
        project,
        name="project",
        out_shape=(
            jax.ShapeDtypeStruct(strip, jnp.float32),
            jax.ShapeDtypeStruct(strip, jnp.bfloat16),
        ),
        in_specs=[smem] + whole(4),
        out_specs=tuple(whole(2)),
        compiler_params=params(),
    )(place, keep, got, value_up, out_proj)
    got = from_partner(send, "kv", 0)
    added = pl.pallas_call(
        add_pair,
        name="add_pair",
        out_shape=jax.ShapeDtypeStruct(strip, jnp.bfloat16),
        in_specs=whole(2),
        out_specs=whole(1)[0],
        compiler_params=params(),
    )(keep, got)
    got = across_chips(added)
    copies = pl.pallas_call(
        normalise,
        name="normalise",
        out_shape=jax.ShapeDtypeStruct(strip, jnp.bfloat16),
        in_specs=whole(3),
        out_specs=whole(1)[0],
        compiler_params=params(),
    )(got, residual, norm_gain.reshape(1, part))
    own = across_chips(copies)
    other = from_partner(own, "kv", 0)

    experts_local = EXPERTS // kv_count
    pick, slot_gate = pl.pallas_call(
        route,
        name="route",
        out_shape=(
            jax.ShapeDtypeStruct((CAP * experts_local, seq_count), jnp.float32),
            jax.ShapeDtypeStruct((CAP, experts_local), jnp.float32),
        ),
        in_specs=[smem] + whole(2),
        out_specs=tuple(whole(2)),
        compiler_params=params(),
    )(place, expert_ids.T, gate_weights.T)
    dispatched, slot_scale = pl.pallas_call(
        finish,
        name="finish",
        out_shape=(
            jax.ShapeDtypeStruct((experts_local, CAP, out_proj.shape[1]), jnp.bfloat16),
            jax.ShapeDtypeStruct((CAP, experts_local), jnp.float32),
        ),
        in_specs=[smem] + whole(3),
        out_specs=tuple(whole(2)),
        compiler_params=params(),
    )(place, own, other, pick)
    return dispatched, slot_scale.T, slot_gate.T


def per_device(*args):
    if lax.axis_size("kv") > H:
        return split_heads(*args)
    return whole_heads(*args)


def solution(mesh):
    in_specs = (
        P("groups", "kv"),
        P("groups", "kv", None),
        P("groups"),
        P("kv", None),
        P("kv", None),
        P("groups", "kv"),
        P("kv"),
        P("groups", None),
        P("groups", None),
    )
    out_specs = (
        P(("groups", "kv"), None, None),
        P(("groups", "kv"), None),
        P(("groups", "kv"), None),
    )
    return jax.shard_map(
        per_device, mesh=mesh, in_specs=in_specs, out_specs=out_specs, check_vma=False
    )
```
